32 devices in a mesh: ens: 8 (over y, x, core), fft: 4 (over z).
Axes of the slice: x: 2, y: 2, z: 4, core: 2. Of those that a mesh axis runs over, the one named last changes fastest.
Arguments:
- field: float32 [16384, 2048], P(('ens', 'fft')), parts along dimension 0, may hold values from -6 to 6
Outputs:
- advanced: float32 [16384, 2048], P(('ens', 'fft')), parts along dimension 0
The draws below stay inside these ranges and needn't reach their ends.
There are 8 independent parts, one for each index of `ens`. The reference program is written for one: setup_inputs(seed, part) draws one part's arguments, and reference() takes and returns one part's arrays. A program takes and returns all parts, laid end to end along the dimension named above; each array names one. Nothing has to cross between parts.
All inputs are finite; a program needn't handle non-finite values.
Results may differ from the reference program's by a relative error of at most 0.000071.
Values sent between devices are 32-bit elements; how exact they have to be, the bound alone decides.
No kernel may reach another device: no remote copies, remote signals or barrier semaphores. Data moves between devices by JAX's collectives and lax.ppermute only.
A program may use at most 192 MiB of HBM per device.

```python
import math
import jax
import jax.numpy as jnp

GRID_POINTS = 2048


def shard_levels(own_key, dims, pieces, low, top_value):
    level, own = 1.0, jax.random.fold_in(own_key, 6)
    for dim, blocks in pieces:
        draws = jnp.exp(jax.random.uniform(jax.random.fold_in(own, dim), (blocks,), jnp.float32, low / len(pieces), top_value / len(pieces)))
        level = level * jnp.repeat(draws, dims[dim] // blocks).reshape([-1 if axis == dim else 1 for axis in range(len(dims))])
    return level


def normal_values(key, extent, scale, bound, shards=(), kind=jnp.bfloat16):
    values = jax.random.normal(key, extent, jnp.float32) * scale
    if len(shards) > 0:
        values = shard_levels(key, extent, shards, -0.22, 0.18) * values
    return jnp.clip(values, min=-bound, max=bound).astype(kind)


def setup_inputs(seed: int = 0, part: int = 0) -> dict:
    keys = jax.random.split(jax.random.key(seed), 2)
    own_keys = jax.random.split(jax.random.fold_in(keys[1], part), 2)
    field = normal_values(own_keys[0], (GRID_POINTS, GRID_POINTS), 1.0, 6.0, ((0, 4),), jnp.float32)
    return dict(field=field)


STEP = 0.05
WAVENUMBER_SCALE = 8.0


def phis(z):
    small = jnp.abs(z) < 1.0
    zs = jnp.where(small, z, 0.0)
    coeffs = [1.0 / math.factorial(n + 3) for n in range(16)]
    third = jnp.zeros_like(z) + coeffs[-1]
    for value in reversed(coeffs[:-1]):
        third = third * zs + value
    second = 0.5 + zs * third
    first = 1.0 + zs * second
    zl = jnp.where(small, -1.0, z)
    first_l = jnp.expm1(zl) / zl
    second_l = (first_l - 1.0) / zl
    third_l = (second_l - 0.5) / zl
    return (jnp.where(small, first, first_l), jnp.where(small, second, second_l), jnp.where(small, third, third_l))


def coefficients(ksq):
    z = STEP * (ksq - ksq * ksq)
    half_one, unused_two, unused_three = phis(0.5 * z)
    one, two, three = phis(z)
    return (jnp.exp(z), jnp.exp(0.5 * z), 0.5 * STEP * half_one, STEP * (one - 3.0 * two + 4.0 * three), STEP * (two - 2.0 * three), STEP * (4.0 * three - two))


def reference(field):
    half_spectrum = GRID_POINTS // 2
    limit = GRID_POINTS // 3
    rows = jnp.arange(GRID_POINTS, dtype=jnp.int32)
    signed_indices = jnp.where(rows < half_spectrum, rows, rows - GRID_POINTS)
    column_indices = jnp.arange(half_spectrum, dtype=jnp.int32)
    mask = ((jnp.abs(signed_indices) < limit)[:, None] & (column_indices < limit)[None, :]).astype(jnp.float32)
    wavenumber_xaxis = jnp.zeros((GRID_POINTS, half_spectrum), jnp.float32) + (signed_indices.astype(jnp.float32) * (WAVENUMBER_SCALE / GRID_POINTS))[:, None]
    wavenumber_yaxis = jnp.zeros((GRID_POINTS, half_spectrum), jnp.float32) + (column_indices.astype(jnp.float32) * (WAVENUMBER_SCALE / GRID_POINTS))[None, :]
    decay, decay_half, q_coef, f_one, f_two, f_three = coefficients(wavenumber_xaxis * wavenumber_xaxis + wavenumber_yaxis * wavenumber_yaxis)

    def forward(grid):
        return mask * jnp.fft.rfft2(grid)[:, :half_spectrum]

    def inverse(spec):
        return jnp.fft.irfft2(jnp.pad(spec, ((0, 0), (0, 1))), s=(GRID_POINTS, GRID_POINTS))

    def nonlinear(spec):
        grad_x = inverse(1j * wavenumber_xaxis * spec)
        grad_y = inverse(1j * wavenumber_yaxis * spec)
        return forward(-0.5 * (grad_x * grad_x + grad_y * grad_y))

    state = forward(field)
    term_v = nonlinear(state)
    section_a = decay_half * state + q_coef * term_v
    term_a = nonlinear(section_a)
    section_b = decay_half * state + q_coef * term_a
    term_b = nonlinear(section_b)
    section_c = decay_half * section_a + q_coef * (2.0 * term_b - term_v)
    term_c = nonlinear(section_c)
    updated = decay * state + f_one * term_v + 2.0 * f_two * (term_a + term_b) + f_three * term_c
    return inverse(updated)
```

```python
import functools
import math

import jax
import jax.numpy as jnp
import numpy as np
from jax import lax
from jax.experimental import pallas as pl
from jax.experimental.pallas import tpu as pltpu
from jax.sharding import PartitionSpec as P

STEP = 0.05
WAVENUMBER_SCALE = 8.0
RADIX = 8
LANES = 128
ROOT = math.sqrt(0.5)
VMEM_LIMIT = 60 * 1024 * 1024
F32 = jnp.float32
BF16 = jnp.bfloat16


def phis(z):
    small = jnp.abs(z) < 1.0
    zs = jnp.where(small, z, 0.0)
    coeffs = [1.0 / math.factorial(n + 3) for n in range(16)]
    third = jnp.zeros_like(z) + coeffs[-1]
    for value in reversed(coeffs[:-1]):
        third = third * zs + value
    second = 0.5 + zs * third
    first = 1.0 + zs * second
    zl = jnp.where(small, -1.0, z)
    first_l = jnp.expm1(zl) / zl
    second_l = (first_l - 1.0) / zl
    third_l = (second_l - 0.5) / zl
    return (
        jnp.where(small, first, first_l),
        jnp.where(small, second, second_l),
        jnp.where(small, third, third_l),
    )


def coefficients(ksq):
    z = STEP * (ksq - ksq * ksq)
    half_one, unused_two, unused_three = phis(0.5 * z)
    one, two, three = phis(z)
    return (
        jnp.exp(z),
        jnp.exp(0.5 * z),
        0.5 * STEP * half_one,
        STEP * (one - 3.0 * two + 4.0 * three),
        STEP * (two - 2.0 * three),
        STEP * (4.0 * three - two),
    )


def round_up(value, step):
    return (value + step - 1) // step * step


class Plan:
    def __init__(self, points):
        self.points = points
        self.block = points // RADIX
        limit = points // 3
        signed = np.arange(-limit + 1, limit)
        of_class = {}
        for residue in (1, 2, 3):
            of_class[residue] = signed[signed % RADIX == residue]
        for residue in (0, 4):
            of_class[residue] = signed[(signed % RADIX == residue) & (signed >= 0)]
        self.parity_classes = ((2, 0, 4), (1, 3))
        joined = [np.concatenate([of_class[r] for r in group]) for group in self.parity_classes]
        self.width = round_up(max(len(one) for one in joined), LANES)
        self.tiles = self.width // LANES
        self.ky = np.zeros((2, self.width), np.int32)
        self.cls = np.full((2, self.width), -1, np.int32)
        for parity, one in enumerate(joined):
            self.ky[parity, : len(one)] = one
            self.cls[parity, : len(one)] = one % RADIX
        self.parts = []
        offset = 0
        for parity, group in enumerate(self.parity_classes):
            for tile in range(self.tiles):
                inside = self.cls[parity, tile * LANES : (tile + 1) * LANES]
                for residue in group:
                    if np.any(inside == residue):
                        size = self.block * (1 if residue in (0, 4) else 2)
                        self.parts.append((parity, tile, residue, offset, size))
                        offset += size
        self.total = offset
        per_class = [signed[signed % RADIX == residue] for residue in range(RADIX)]
        self.count = round_up(max(len(one) for one in per_class), 16)
        self.kx = np.zeros((RADIX, self.count), np.int32)
        self.kx_live = np.zeros((RADIX, self.count), np.float32)
        for residue, one in enumerate(per_class):
            self.kx[residue, : len(one)] = one
            self.kx_live[residue, : len(one)] = 1.0
        self.rows = RADIX * self.count


def hi_lo(table):
    high = lax.reduce_precision(table, 8, 7)
    return high.astype(BF16), (table - high).astype(BF16)


def waves(points, left, right):
    product = (left * right) & (points - 1)
    angle = product.astype(F32) * (2.0 * math.pi / points)
    return jnp.cos(angle), jnp.sin(angle)


def y_tables(plan):
    n = jnp.arange(plan.block, dtype=jnp.int32)
    ky = jnp.asarray(plan.ky.reshape(-1))
    cos, sin = waves(plan.points, n[:, None], ky[None, :])
    weight = np.where(plan.ky.reshape(-1) == 0, 1.0, 2.0) / (plan.points * plan.points)
    weight = jnp.asarray(weight.astype(np.float32))
    forward, grad, plain = [], [], []
    for parity, tile, residue, unused_offset, unused_size in plan.parts:
        start = parity * plan.width + tile * LANES
        live = (plan.cls.reshape(-1)[start : start + LANES] == residue).astype(np.float32)
        c = cos[:, start : start + LANES] * live
        s = sin[:, start : start + LANES] * live
        w = weight[start : start + LANES]
        ct = (c * w).T
        st = (s * w).T
        top = jnp.concatenate([c, -s], axis=1)
        if residue in (0, 4):
            forward.append(top)
            plain.append(jnp.concatenate([ct, -st], axis=0))
            grad.append(jnp.concatenate([-st, -ct], axis=0))
        else:
            forward.append(jnp.concatenate([top, jnp.concatenate([s, c], axis=1)], axis=0))
            up = jnp.concatenate([ct, -st], axis=0)
            down = jnp.concatenate([st, ct], axis=0)
            plain.append(jnp.concatenate([up, down], axis=1))
            up = jnp.concatenate([-st, -ct], axis=0)
            down = jnp.concatenate([ct, -st], axis=0)
            grad.append(jnp.concatenate([up, down], axis=1))
    return (
        hi_lo(jnp.concatenate(forward, axis=0)),
        hi_lo(jnp.concatenate(grad, axis=1)),
        hi_lo(jnp.concatenate(plain, axis=1)),
    )


def x_tables(plan):
    n = jnp.arange(plan.block, dtype=jnp.int32)
    kx = jnp.asarray(plan.kx)
    cos, sin = waves(plan.points, kx[:, :, None], n[None, None, :])
    live = jnp.asarray(plan.kx_live)[:, :, None]
    cos = cos * live
    sin = sin * live
    forward = jnp.concatenate([cos, sin], axis=1)
    inverse = jnp.concatenate([cos.transpose(0, 2, 1), sin.transpose(0, 2, 1)], axis=1)
    return hi_lo(forward), hi_lo(inverse)


def split(value):
    high = value.astype(BF16)
    return high, (value - high.astype(F32)).astype(BF16)


def dot(left, right):
    return jnp.dot(left, right, preferred_element_type=F32)


def dot3(left, right):
    lh, ll = left
    rh, rl = right
    return dot(lh, rh) + dot(lh, rl) + dot(ll, rh)


def y_forward_values(plan, blocks, table_hi, table_lo):
    p = [blocks[q] + blocks[q + 4] for q in range(4)]
    m = [blocks[q] - blocks[q + 4] for q in range(4)]
    even = p[0] + p[2]
    odd = p[1] + p[3]
    minus = ROOT * (m[1] - m[3])
    plus = ROOT * (m[1] + m[3])
    classes = {
        0: even + odd,
        4: even - odd,
        2: jnp.concatenate([p[0] - p[2], p[3] - p[1]], axis=1),
        1: jnp.concatenate([m[0] + minus, -m[2] - plus], axis=1),
        3: jnp.concatenate([m[0] - minus, m[2] - plus], axis=1),
    }
    parts = {residue: split(value) for residue, value in classes.items()}
    out = {}
    for parity, tile, residue, offset, size in plan.parts:
        table = (table_hi[offset : offset + size, :], table_lo[offset : offset + size, :])
        value = dot3(parts[residue], table)
        key = (parity, tile)
        out[key] = out[key] + value if key in out else value
    return out


def y_inverse_values(plan, tiles, table_hi, table_lo):
    parts = {key: split(value) for key, value in tiles.items()}
    z = {}
    for parity, tile, residue, offset, size in plan.parts:
        table = (table_hi[:, offset : offset + size], table_lo[:, offset : offset + size])
        value = dot3(parts[(parity, tile)], table)
        z[residue] = z[residue] + value if residue in z else value
    block = plan.block
    a1, b1 = z[1][:, :block], z[1][:, block:]
    a2, b2 = z[2][:, :block], z[2][:, block:]
    a3, b3 = z[3][:, :block], z[3][:, block:]
    u = z[0] + z[4]
    v = z[0] - z[4]
    even = [u + a2, v - b2, u - a2, v + b2]
    s = a1 - a3
    t = b1 + b3
    odd = [a1 + a3, ROOT * (s - t), b3 - b1, -ROOT * (s + t)]
    return [even[q] + odd[q] for q in range(4)] + [even[q] - odd[q] for q in range(4)]


def store_pair(flag, out, first, second, tiles):
    for tile in range(tiles):
        even, odd = out[(0, tile)], out[(1, tile)]
        lanes = slice(tile * LANES, (tile + 1) * LANES)
        one = jnp.where(flag == 0, even, odd)
        two = jnp.where(flag == 0, odd, even)
        first[0, :, lanes] = one[:, :LANES]
        first[1, :, lanes] = one[:, LANES:]
        second[0, :, lanes] = two[:, :LANES]
        second[1, :, lanes] = two[:, LANES:]


def load_pair(flag, own, other, tiles):
    out = {}
    for tile in range(tiles):
        lanes = slice(tile * LANES, (tile + 1) * LANES)
        mine = jnp.concatenate([own[0, :, lanes], own[1, :, lanes]], axis=1)
        its = jnp.concatenate([other[0, :, lanes], other[1, :, lanes]], axis=1)
        out[(0, tile)] = jnp.where(flag == 0, mine, its)
        out[(1, tile)] = jnp.where(flag == 0, its, mine)
    return out


def y_first_kernel(plan, flag, grid, fh, fl, first, second):
    block = plan.block
    blocks = [grid[:, q * block : (q + 1) * block] for q in range(RADIX)]
    out = y_forward_values(plan, blocks, fh, fl)
    store_pair(flag[0], out, first, second, plan.tiles)


def y_middle_kernel(plan, flag, ky, po, pr, qo, qr, gh, gl, fh, fl, first, second):
    tiles = load_pair(flag[0], qo, qr, plan.tiles)
    gx = y_inverse_values(plan, tiles, gh, gl)
    square = [value * value for value in gx]
    tiles = load_pair(flag[0], po, pr, plan.tiles)
    scaled = {}
    for (parity, tile), value in tiles.items():
        row = ky[parity : parity + 1, tile * LANES : (tile + 1) * LANES]
        scaled[(parity, tile)] = value * jnp.concatenate([row, row], axis=1)
    gy = y_inverse_values(plan, scaled, gh, gl)
    square = [one + two * two for one, two in zip(square, gy)]
    out = y_forward_values(plan, square, fh, fl)
    store_pair(flag[0], out, first, second, plan.tiles)


def y_last_kernel(plan, count, flag, *refs):
    received, (ph, plo, grid) = refs[:count], refs[count:]
    place = flag[0]
    tiles = {}
    for tile in range(plan.tiles):
        lanes = slice(tile * LANES, (tile + 1) * LANES)
        loaded = [jnp.concatenate([r[0, :, lanes], r[1, :, lanes]], axis=1) for r in received]
        even, odd = loaded[0], loaded[count // 2]
        for k in range(1, count):
            even = jnp.where(place == k, loaded[k], even)
            odd = jnp.where(place == k, loaded[(k + count // 2) % count], odd)
        tiles[(0, tile)] = even
        tiles[(1, tile)] = odd
    blocks = y_inverse_values(plan, tiles, ph, plo)
    for q in range(RADIX):
        grid[:, q * plan.block : (q + 1) * plan.block] = blocks[q]


def turn(value):
    return jnp.concatenate([value[:, LANES:], -value[:, :LANES]], axis=1)


def unturn(value):
    return jnp.concatenate([-value[:, LANES:], value[:, :LANES]], axis=1)


def butterfly(x, rotate):
    p = [x[q] + x[q + 4] for q in range(4)]
    m = [x[q] - x[q + 4] for q in range(4)]
    s0, s1 = p[0] + p[2], p[1] + p[3]
    d0, d1 = p[0] - p[2], rotate(p[1] - p[3])
    a = ROOT * (m[1] - m[3])
    b = rotate(ROOT * (m[1] + m[3]))
    c = rotate(m[2])
    top, low = m[0] + c, m[0] - c
    plus, minus = a + b, a - b
    return [
        s0 + s1,
        top + plus,
        d0 + d1,
        low - minus,
        s0 - s1,
        top - plus,
        d0 - d1,
        low + minus,
    ]


def x_forward_values(plan, x, table_hi, table_lo):
    count = plan.count
    out = []
    for residue, value in enumerate(butterfly(x, turn)):
        both = dot3((table_hi[residue], table_lo[residue]), split(value))
        out.append(both[:count] + turn(both[count:]))
    return out


def x_inverse_values(plan, spec, table_hi, table_lo):
    block = plan.block
    z = []
    for residue in range(RADIX):
        both = dot3((table_hi[residue], table_lo[residue]), split(spec[residue]))
        z.append(both[:block] + unturn(both[block:]))
    return butterfly(z, unturn)


def choose(flag, values, partner):
    return [jnp.where(flag == 0, values[q], values[partner[q]]) for q in range(RADIX)]


def x_kernel(plan, mode, partner, out_partner, out_rows, flag, *refs):
    refs = list(refs)

    def take(number):
        head = refs[:number]
        del refs[:number]
        return head

    inputs = take(RADIX)
    fh, fl, ih, il = take(4)
    (kx,) = take(1)
    state_in = take({"state": 0, "v": 1, "a": 2, "b": 2, "c": 1}[mode])
    coef = take({"state": 0, "v": 4, "a": 3, "b": 2, "c": 1}[mode])
    state_out = take({"state": 1, "v": 2, "a": 1, "b": 1, "c": 0}[mode])
    fields = refs
    place = flag[0]
    loaded = [jnp.concatenate([r[0], r[1]], axis=1) for r in inputs]
    x = choose(place, loaded, partner)
    spec = x_forward_values(plan, x, fh, fl)
    count = plan.count
    fresh = []
    for residue in range(RADIX):
        rows = slice(residue * count, (residue + 1) * count)

        def read(ref):
            return jnp.concatenate([ref[0, rows, :], ref[1, rows, :]], axis=1)

        def factor(ref):
            return jnp.concatenate([ref[rows, :], ref[rows, :]], axis=1)

        def write(ref, value):
            ref[0, rows, :] = value[:, :LANES]
            ref[1, rows, :] = value[:, LANES:]

        term = spec[residue]
        if mode == "state":
            write(state_out[0], term)
            fresh.append(term)
        elif mode == "v":
            v = read(state_in[0])
            full, half, q, one = [factor(r) for r in coef]
            pushed = q * term
            a = half * v + pushed
            write(state_out[0], half * a - pushed)
            write(state_out[1], full * v + one * term)
            fresh.append(a)
        elif mode == "a":
            half, q, two = [factor(r) for r in coef]
            fresh.append(half * read(state_in[0]) + q * term)
            write(state_out[0], read(state_in[1]) + two * term)
        elif mode == "b":
            q, two = [factor(r) for r in coef]
            fresh.append(read(state_in[0]) + (2.0 * q) * term)
            write(state_out[0], read(state_in[1]) + two * term)
        else:
            fresh.append(read(state_in[0]) + factor(coef[0]) * term)

    def put(targets, values):
        values = choose(place, values, out_partner)
        for q in range(RADIX):
            which, row = out_rows[q]
            target = targets[which]
            target[0, row : row + plan.block, :] = values[q][:, :LANES]
            target[1, row : row + plan.block, :] = values[q][:, LANES:]

    if mode == "c":
        put(fields, x_inverse_values(plan, fresh, ih, il))
    else:
        put(fields[:2], x_inverse_values(plan, fresh, ih, il))
        for residue in range(RADIX):
            wave = kx[residue * count : (residue + 1) * count, :]
            fresh[residue] = fresh[residue] * jnp.concatenate([wave, wave], axis=1)
        put(fields[2:], x_inverse_values(plan, fresh, ih, il))


SCALAR = pl.BlockSpec(memory_space=pltpu.SMEM)


def fixed(shape):
    zero = (0,) * len(shape)
    return pl.BlockSpec(shape, lambda i: zero, pipeline_mode=pl.Buffered(1))


def params():
    return pltpu.CompilerParams(
        dimension_semantics=("arbitrary",), vmem_limit_bytes=VMEM_LIMIT
    )


def row_tile(rows):
    tile = min(rows, 256)
    return tile if rows % tile == 0 else rows


def pair_shape(rows, width):
    return jax.ShapeDtypeStruct((2, rows, width), F32)


def pair_spec(tile, width):
    return pl.BlockSpec((2, tile, width), lambda i: (0, i, 0))


def y_first(plan, flag, grid, forward):
    rows = grid.shape[0]
    tile = row_tile(rows)
    return pl.pallas_call(
        functools.partial(y_first_kernel, plan),
        name="y_first",
        grid=(rows // tile,),
        in_specs=[
            SCALAR,
            pl.BlockSpec((tile, plan.points), lambda i: (i, 0)),
            fixed(forward[0].shape),
            fixed(forward[1].shape),
        ],
        out_specs=[pair_spec(tile, plan.width)] * 2,
        out_shape=[pair_shape(rows, plan.width)] * 2,
        compiler_params=params(),
    )(flag, grid, *forward)


def y_middle(plan, flag, ky, fields, grad, forward):
    rows = fields[0].shape[1]
    tile = row_tile(rows)
    return pl.pallas_call(
        functools.partial(y_middle_kernel, plan),
        name="y_middle",
        grid=(rows // tile,),
        in_specs=[SCALAR, fixed(ky.shape)]
        + [pair_spec(tile, plan.width)] * 4
        + [fixed(t.shape) for t in (*grad, *forward)],
        out_specs=[pair_spec(tile, plan.width)] * 2,
        out_shape=[pair_shape(rows, plan.width)] * 2,
        compiler_params=params(),
    )(flag, ky, *fields, *grad, *forward)


def y_last(plan, flag, pieces, plain):
    rows = pieces[0].shape[1]
    tile = row_tile(rows)
    return pl.pallas_call(
        functools.partial(y_last_kernel, plan, len(pieces)),
        name="y_last",
        grid=(rows // tile,),
        in_specs=[SCALAR]
        + [pair_spec(tile, plan.width)] * len(pieces)
        + [fixed(t.shape) for t in plain],
        out_specs=pl.BlockSpec((tile, plan.points), lambda i: (i, 0)),
        out_shape=jax.ShapeDtypeStruct((rows, plan.points), F32),
        compiler_params=params(),
    )(flag, *pieces, *plain)


def x_stage(plan, mode, flag, inputs, partner, tables, kx, state, coef, out_rows, out_partner, sizes):
    def rows_at(place):
        return pl.BlockSpec((2, plan.block, LANES), lambda i: (0, place, i))

    spectrum = pl.BlockSpec((2, plan.rows, LANES), lambda i: (0, 0, i))
    factor = pl.BlockSpec((plan.rows, LANES), lambda i: (0, i))
    kept = {"state": 1, "v": 2, "a": 1, "b": 1, "c": 0}[mode]
    return pl.pallas_call(
        functools.partial(x_kernel, plan, mode, partner, out_partner, out_rows),
        name="x_" + mode,
        grid=(plan.tiles,),
        in_specs=[SCALAR]
        + [rows_at(place) for unused_array, place in inputs]
        + [fixed(t.shape) for t in tables]
        + [fixed(kx.shape)]
        + [spectrum] * len(state)
        + [factor] * len(coef),
        out_specs=[spectrum] * kept
        + [pl.BlockSpec((2, size, LANES), lambda i: (0, 0, i)) for size in sizes],
        out_shape=[pair_shape(plan.rows, plan.width)] * kept
        + [pair_shape(size, plan.width) for size in sizes],
        compiler_params=params(),
    )(flag, *[array for array, unused_place in inputs], *tables, kx, *state, *coef)


def on_device(members, devices, field):
    plan = Plan(field.shape[1])
    rows = field.shape[0]
    half = devices // 2
    core = lax.axis_index("ens") % 2
    place = lax.axis_index("fft")
    core_flag = core.astype(jnp.int32).reshape(1)
    place_flag = place.astype(jnp.int32).reshape(1)
    side_flag = (place >= half).astype(jnp.int32).reshape(1)

    forward, grad, plain = y_tables(plan)
    x_forward, x_inverse = x_tables(plan)
    tables = (*x_forward, *x_inverse)
    scale = WAVENUMBER_SCALE / plan.points
    wave_y = jnp.asarray(plan.ky.astype(np.float32) * np.float32(scale))
    wave_x = jnp.asarray(plan.kx.reshape(-1).astype(np.float32) * np.float32(scale))
    own_y = jnp.where(core == 0, wave_y[0], wave_y[1])
    kx = jnp.broadcast_to(wave_x[:, None], (plan.rows, LANES))
    ksq = (wave_x * wave_x)[:, None] + (own_y * own_y)[None, :]
    decay, decay_half, q_coef, f_one, f_two, f_three = coefficients(ksq)
    q_coef = -0.5 * q_coef
    f_one = -0.5 * f_one
    f_two = -f_two
    f_three = -0.5 * f_three

    def index(member, at):
        return member * devices + at

    def gather_pairs(k):
        pairs = []
        for base in range(0, members, 2):
            for which in range(2):
                for to_core in range(2):
                    source = (k + to_core * half) % devices
                    pairs.append((index(base + which, source), index(base + to_core, half - 1 + which)))
        return pairs

    sibling = [
        (index(m, at), index(m ^ 1, at)) for m in range(members) for at in range(devices)
    ]
    axes = ("ens", "fft")
    first, second = y_first(plan, side_flag, field, forward)
    pieces = [
        lax.ppermute(first if k < half else second, axes, gather_pairs(k)) for k in range(devices)
    ]
    per = rows // plan.block
    opposite = tuple((q + RADIX // 2) % RADIX for q in range(RADIX))
    beside = tuple(q ^ 1 for q in range(RADIX))
    share = plan.points // 2
    near = tuple((q % 2, q // 2 * plan.block) for q in range(RADIX))

    def x_first():
        inputs = [(pieces[q // per], q % per) for q in range(RADIX)]
        return x_stage(
            plan, "state", core_flag, inputs, opposite, tables, kx, (), (), near, beside, (share,) * 4
        )

    def nonlinear(fields, mode, state, coef):
        po, ps, qo, qs = fields
        pr = lax.ppermute(ps, axes, sibling)
        qr = lax.ppermute(qs, axes, sibling)
        own, send = y_middle(plan, core_flag, wave_y, (po, pr, qo, qr), grad, forward)
        received = lax.ppermute(send, axes, sibling)
        inputs = [(received if q % 2 else own, q // 2) for q in range(RADIX)]
        if mode == "c":
            out_rows = tuple((q // per, q % per * plan.block) for q in range(RADIX))
            sizes = (rows,) * devices
            return x_stage(
                plan, mode, core_flag, inputs, beside, tables, kx, state, coef, out_rows, opposite, sizes
            )
        return x_stage(
            plan, mode, core_flag, inputs, beside, tables, kx, state, coef, near, beside, (share,) * 4
        )

    v, *fields = x_first()
    c_part, total, *fields = nonlinear(fields, "v", (v,), (decay, decay_half, q_coef, f_one))
    total, *fields = nonlinear(fields, "a", (v, total), (decay_half, q_coef, f_two))
    total, *fields = nonlinear(fields, "b", (c_part, total), (q_coef, f_two))
    outputs = nonlinear(fields, "c", (total,), (f_three,))
    received = [
        lax.ppermute(outputs[k], axes, [(to, source) for source, to in gather_pairs(k)])
        for k in range(devices)
    ]
    return y_last(plan, place_flag, received, plain)


def solution(mesh):
    members = mesh.shape["ens"]
    devices = mesh.shape["fft"]
    return jax.shard_map(
        functools.partial(on_device, members, devices),
        mesh=mesh,
        in_specs=(P(("ens", "fft"), None),),
        out_specs=P(("ens", "fft"), None),
        check_vma=False,
    )
```

```python
import functools
import math

import jax
import jax.numpy as jnp
import numpy as np
from jax import lax
from jax.experimental import pallas as pl
from jax.experimental.pallas import tpu as pltpu
from jax.sharding import PartitionSpec as P

STEP = 0.05
WAVENUMBER_SCALE = 8.0
RADIX = 8
Y_RADIX = 16
LANES = 128
ROOT = math.sqrt(0.5)
BIG = math.cos(math.pi / 8)
TINY = math.sin(math.pi / 8)
VMEM_LIMIT = 60 * 1024 * 1024
F32 = jnp.float32
BF16 = jnp.bfloat16


def phis(z):
    small = jnp.abs(z) < 1.0
    zs = jnp.where(small, z, 0.0)
    coeffs = [1.0 / math.factorial(n + 3) for n in range(16)]
    third = jnp.zeros_like(z) + coeffs[-1]
    for value in reversed(coeffs[:-1]):
        third = third * zs + value
    second = 0.5 + zs * third
    first = 1.0 + zs * second
    zl = jnp.where(small, -1.0, z)
    first_l = jnp.expm1(zl) / zl
    second_l = (first_l - 1.0) / zl
    third_l = (second_l - 0.5) / zl
    return (
        jnp.where(small, first, first_l),
        jnp.where(small, second, second_l),
        jnp.where(small, third, third_l),
    )


def coefficients(ksq):
    z = STEP * (ksq - ksq * ksq)
    half_one, unused_two, unused_three = phis(0.5 * z)
    one, two, three = phis(z)
    return (
        jnp.exp(z),
        jnp.exp(0.5 * z),
        0.5 * STEP * half_one,
        STEP * (one - 3.0 * two + 4.0 * three),
        STEP * (two - 2.0 * three),
        STEP * (4.0 * three - two),
    )


def round_up(value, step):
    return (value + step - 1) // step * step


class Plan:
    def __init__(self, points):
        self.points = points
        limit = points // 3
        signed = np.arange(-limit + 1, limit)
        self.y_block = points // Y_RADIX
        of_class = {r: signed[signed % Y_RADIX == r] for r in range(1, Y_RADIX // 2)}
        for r in (0, Y_RADIX // 2):
            of_class[r] = signed[(signed % Y_RADIX == r) & (signed >= 0)]
        self.groups = (((2,), (4,), (6,), (0, 8)), ((1,), (3,), (5,), (7,)))
        joined = [[np.concatenate([of_class[r] for r in group]) for group in one] for one in self.groups]
        self.used = max(len(one) for parity in joined for one in parity)
        self.tile = round_up(self.used, LANES)
        self.third = -(-self.used // 3)
        self.tiles = 3
        self.width = self.tiles * self.tile
        self.lane_ky = np.zeros((2, 4, self.tile), np.int32)
        self.lane_class = np.full((2, 4, self.tile), -1, np.int32)
        self.ky = np.zeros((2, self.width), np.int32)
        self.places = (self.used, 0, self.third)
        for parity in range(2):
            for group in range(3):
                one = joined[parity][group]
                self.lane_ky[parity, group, : len(one)] = one
                self.lane_class[parity, group, : len(one)] = one % Y_RADIX
                self.ky[parity, group * self.tile : group * self.tile + len(one)] = one
            for piece in range(3):
                one = joined[parity][3][piece * self.third : (piece + 1) * self.third]
                at = self.places[piece]
                self.lane_ky[parity, 3, at : at + len(one)] = one
                self.lane_class[parity, 3, at : at + len(one)] = one % Y_RADIX
                at = piece * self.tile + self.used
                self.ky[parity, at : at + len(one)] = one
        self.block = points // RADIX
        per_class = [signed[signed % RADIX == residue] for residue in range(RADIX)]
        self.count = round_up(max(len(one) for one in per_class), 16)
        self.kx = np.zeros((RADIX, self.count), np.int32)
        self.kx_live = np.zeros((RADIX, self.count), np.float32)
        for residue, one in enumerate(per_class):
            self.kx[residue, : len(one)] = one
            self.kx_live[residue, : len(one)] = 1.0
        self.rows = RADIX * self.count


def hi_lo(table):
    high = lax.reduce_precision(table, 8, 7)
    return high.astype(BF16), (table - high).astype(BF16)


def waves(points, left, right):
    product = (left * right) & (points - 1)
    angle = product.astype(F32) * (2.0 * math.pi / points)
    return jnp.cos(angle), jnp.sin(angle)


def y_parts(plan, xp, cos, sin):
    out = []
    for parity in range(2):
        for group in range(4):
            at = (parity * 4 + group) * plan.tile
            c, s = cos[:, at : at + plan.tile], sin[:, at : at + plan.tile]
            cls = plan.lane_class[parity, group]
            if group == 3 and parity == 0:
                low = (cls == 0).astype(np.float32)
                high = (cls == Y_RADIX // 2).astype(np.float32)
                out.append((True, c * low, s * low, c * high, s * high))
            else:
                live = (cls >= 0).astype(np.float32)
                out.append((False, c * live, s * live, None, None))
    return out


def y_forward_table(plan):
    n = np.arange(plan.y_block, dtype=np.int64)
    ky = plan.lane_ky.reshape(-1).astype(np.int64)
    angle = (n[:, None] * ky[None, :] % plan.points) * (2.0 * math.pi / plan.points)
    blocks = []
    for real, c, s, c8, s8 in y_parts(plan, np, np.cos(angle), np.sin(angle)):
        top = np.concatenate([c, -s], axis=1)
        low = np.concatenate([c8, -s8] if real else [s, c], axis=1)
        blocks.append(np.concatenate([top, low], axis=0))
    table = np.stack(blocks)
    high = table.astype(BF16)
    low = (table - high.astype(np.float64)).astype(BF16)
    return jnp.asarray(high), jnp.asarray(low)


def y_inverse_tables(plan):
    n = jnp.arange(plan.y_block, dtype=jnp.int32)
    ky = jnp.asarray(plan.lane_ky.reshape(-1))
    cos, sin = waves(plan.points, ky[:, None], n[None, :])
    weight = np.where(plan.lane_ky.reshape(-1) == 0, 1.0, 2.0) / (plan.points * plan.points)
    low = np.where(plan.lane_class == Y_RADIX // 2, 0.0, 1.0)
    low = np.where(plan.lane_class < 0, 0.0, low).reshape(-1) * weight
    high = np.where(plan.lane_class == Y_RADIX // 2, weight.reshape(plan.lane_class.shape), 0.0)
    real = np.zeros(plan.lane_class.shape, bool)
    real[0, 3] = True
    real = real.reshape(-1)
    low = jnp.asarray(low.astype(np.float32))[:, None]
    high = jnp.asarray(high.reshape(-1).astype(np.float32))[:, None]
    real = jnp.asarray(real)[:, None]
    c, s, ch, sh = cos * low, sin * low, cos * high, sin * high
    shape = (8, plan.tile, plan.y_block)

    def corner(complex_value, real_value):
        return jnp.where(real, real_value, complex_value).reshape(shape)

    def build(a, b, d, e):
        up = jnp.concatenate([a, b], axis=2)
        down = jnp.concatenate([d, e], axis=2)
        return hi_lo(jnp.concatenate([up, down], axis=1))

    plain = build(c.reshape(shape), corner(s, ch), (-s).reshape(shape), corner(c, -sh))
    grad = build((-s).reshape(shape), corner(c, -sh), (-c).reshape(shape), corner(-s, -ch))
    return grad, plain


def x_tables(plan):
    n = jnp.arange(plan.block, dtype=jnp.int32)
    kx = jnp.asarray(plan.kx)
    cos, sin = waves(plan.points, kx[:, :, None], n[None, None, :])
    live = jnp.asarray(plan.kx_live)[:, :, None]
    cos = cos * live
    sin = sin * live
    forward = jnp.concatenate([cos, sin], axis=1)
    inverse = jnp.concatenate([cos.transpose(0, 2, 1), sin.transpose(0, 2, 1)], axis=1)
    return hi_lo(forward), hi_lo(inverse)


def split(value):
    high = value.astype(BF16)
    return high, (value - high.astype(F32)).astype(BF16)


def dot(left, right):
    return jnp.dot(left, right, preferred_element_type=F32)


def dot3(left, right):
    lh, ll = left
    rh, rl = right
    return dot(lh, rh) + dot(lh, rl) + dot(ll, rh)


def real_forward(x):
    p = [x[q] + x[q + 4] for q in range(4)]
    m = [x[q] - x[q + 4] for q in range(4)]
    even = p[0] + p[2]
    odd = p[1] + p[3]
    minus = ROOT * (m[1] - m[3])
    plus = ROOT * (m[1] + m[3])
    return (
        even + odd,
        even - odd,
        (m[0] + minus, -m[2] - plus),
        (p[0] - p[2], p[3] - p[1]),
        (m[0] - minus, m[2] - plus),
    )


def real_inverse(z0, z4, z1, z2, z3):
    u, v = z0 + z4, z0 - z4
    even = [u + z2[0], v - z2[1], u - z2[0], v + z2[1]]
    s, t = z1[0] - z3[0], z1[1] + z3[1]
    odd = [z1[0] + z3[0], ROOT * (s - t), z3[1] - z1[1], -ROOT * (s + t)]
    return [even[q] + odd[q] for q in range(4)] + [even[q] - odd[q] for q in range(4)]


def lanes_of(value):
    return lax.broadcasted_iota(jnp.int32, value.shape, 1)


def y_forward_values(plan, x, table_hi, table_lo):
    p = [x[q] + x[q + 8] for q in range(8)]
    m = [x[q] - x[q + 8] for q in range(8)]
    z0, z8, z2, z4, z6 = real_forward(p)
    a = [m[q] - m[8 - q] for q in (1, 2, 3)]
    b = [m[q] + m[8 - q] for q in (1, 2, 3)]
    first, last = m[0] + ROOT * a[1], m[0] - ROOT * a[1]
    u, v = BIG * a[0] + TINY * a[2], TINY * a[0] - BIG * a[2]
    g, h = m[4] + ROOT * b[1], m[4] - ROOT * b[1]
    s, t = TINY * b[0] + BIG * b[2], BIG * b[0] - TINY * b[2]
    groups = [
        [z2, z4, z6, (z0, z8)],
        [(first + u, -g - s), (last + v, h - t), (last - v, -h - t), (first - u, g - s)],
    ]
    out = {}
    for parity in range(2):
        values = []
        for group in range(4):
            k = parity * 4 + group
            data = split(jnp.concatenate(groups[parity][group], axis=1))
            both = dot3(data, (table_hi[k], table_lo[k]))
            values.append((both[:, : plan.tile], both[:, plan.tile :]))
        lane = lanes_of(values[3][0])
        inside = (lane >= plan.used) & (lane < plan.used + plan.third)
        for tile in range(3):
            shift = (plan.used - plan.places[tile]) % plan.tile
            pair = []
            for part in range(2):
                extra = values[3][part]
                if shift:
                    extra = pltpu.roll(extra, shift, 1)
                pair.append(jnp.where(inside, extra, values[tile][part]))
            out[(parity, tile)] = tuple(pair)
    return out


def y_inverse_values(plan, tiles, table_hi, table_lo):
    z = []
    for parity in range(2):
        extra = []
        for part in range(2):
            value = [tiles[(parity, tile)][part] for tile in range(3)]
            lane = lanes_of(value[0])
            one = pltpu.roll(value[1], plan.tile - plan.used, 1)
            two = pltpu.roll(value[2], plan.tile - plan.used + plan.third, 1)
            extra.append(jnp.where(lane >= plan.used, value[0], jnp.where(lane < plan.third, one, two)))
        for group in range(4):
            k = parity * 4 + group
            pair = tuple(extra) if group == 3 else tiles[(parity, group)]
            both = dot3(split(jnp.concatenate(pair, axis=1)), (table_hi[k], table_lo[k]))
            z.append((both[:, : plan.y_block], both[:, plan.y_block :]))
    z2, z4, z6, (z0, z8), z1, z3, z5, z7 = z
    even = real_inverse(z0, z8, z2, z4, z6)
    r17, r35 = z1[0] + z7[0], z3[0] + z5[0]
    d17, d35 = z1[0] - z7[0], z3[0] - z5[0]
    i17, i35 = z1[1] + z7[1], z3[1] + z5[1]
    j17, j35 = z1[1] - z7[1], z3[1] - z5[1]
    c1, c2, c3 = BIG * d17 + TINY * d35, ROOT * (r17 - r35), TINY * d17 - BIG * d35
    s1, s2, s3 = TINY * i17 + BIG * i35, ROOT * (j17 + j35), BIG * i17 - TINY * i35
    odd = [r17 + r35, c1 - s1, c2 - s2, c3 - s3, j35 - j17, -c3 - s3, -c2 - s2, -c1 - s1]
    return [even[q] + odd[q] for q in range(8)] + [even[q] - odd[q] for q in range(8)]


def store_pair(plan, flag, out, first, second):
    for tile in range(plan.tiles):
        lanes = slice(tile * plan.tile, (tile + 1) * plan.tile)
        for part in range(2):
            even, odd = out[(0, tile)][part], out[(1, tile)][part]
            first[part, :, lanes] = jnp.where(flag == 0, even, odd)
            second[part, :, lanes] = jnp.where(flag == 0, odd, even)


def load_pair(plan, flag, own, other):
    out = {}
    for tile in range(plan.tiles):
        lanes = slice(tile * plan.tile, (tile + 1) * plan.tile)
        mine = (own[0, :, lanes], own[1, :, lanes])
        its = (other[0, :, lanes], other[1, :, lanes])
        out[(0, tile)] = tuple(jnp.where(flag == 0, a, b) for a, b in zip(mine, its))
        out[(1, tile)] = tuple(jnp.where(flag == 0, b, a) for a, b in zip(mine, its))
    return out


def y_first_kernel(plan, flag, grid, fh, fl, first, second):
    block = plan.y_block
    blocks = [grid[:, q * block : (q + 1) * block] for q in range(Y_RADIX)]
    store_pair(plan, flag[0], y_forward_values(plan, blocks, fh, fl), first, second)


def y_middle_kernel(plan, flag, ky, po, pr, qo, qr, gh, gl, fh, fl, first, second):
    gx = y_inverse_values(plan, load_pair(plan, flag[0], qo, qr), gh, gl)
    square = [value * value for value in gx]
    tiles = load_pair(plan, flag[0], po, pr)
    scaled = {}
    for (parity, tile), pair in tiles.items():
        row = ky[parity : parity + 1, tile * plan.tile : (tile + 1) * plan.tile]
        scaled[(parity, tile)] = tuple(value * row for value in pair)
    gy = y_inverse_values(plan, scaled, gh, gl)
    square = [one + two * two for one, two in zip(square, gy)]
    store_pair(plan, flag[0], y_forward_values(plan, square, fh, fl), first, second)


def y_last_kernel(plan, count, flag, *refs):
    received, (ph, plo, grid) = refs[:count], refs[count:]
    place = flag[0]
    tiles = {}
    for tile in range(plan.tiles):
        lanes = slice(tile * plan.tile, (tile + 1) * plan.tile)
        pairs = ([], [])
        for part in range(2):
            loaded = [r[part, :, lanes] for r in received]
            even, odd = loaded[0], loaded[count // 2]
            for k in range(1, count):
                even = jnp.where(place == k, loaded[k], even)
                odd = jnp.where(place == k, loaded[(k + count // 2) % count], odd)
            pairs[0].append(even)
            pairs[1].append(odd)
        tiles[(0, tile)] = tuple(pairs[0])
        tiles[(1, tile)] = tuple(pairs[1])
    blocks = y_inverse_values(plan, tiles, ph, plo)
    for q in range(Y_RADIX):
        grid[:, q * plan.y_block : (q + 1) * plan.y_block] = blocks[q]


def turn(value):
    return jnp.concatenate([value[:, LANES:], -value[:, :LANES]], axis=1)


def unturn(value):
    return jnp.concatenate([-value[:, LANES:], value[:, :LANES]], axis=1)


def butterfly(x, rotate):
    p = [x[q] + x[q + 4] for q in range(4)]
    m = [x[q] - x[q + 4] for q in range(4)]
    s0, s1 = p[0] + p[2], p[1] + p[3]
    d0, d1 = p[0] - p[2], rotate(p[1] - p[3])
    a = ROOT * (m[1] - m[3])
    b = rotate(ROOT * (m[1] + m[3]))
    c = rotate(m[2])
    top, low = m[0] + c, m[0] - c
    plus, minus = a + b, a - b
    return [
        s0 + s1,
        top + plus,
        d0 + d1,
        low - minus,
        s0 - s1,
        top - plus,
        d0 - d1,
        low + minus,
    ]


def x_forward_values(plan, x, table_hi, table_lo):
    count = plan.count
    out = []
    for residue, value in enumerate(butterfly(x, turn)):
        both = dot3((table_hi[residue], table_lo[residue]), split(value))
        out.append(both[:count] + turn(both[count:]))
    return out


def x_inverse_values(plan, spec, table_hi, table_lo):
    block = plan.block
    z = []
    for residue in range(RADIX):
        both = dot3((table_hi[residue], table_lo[residue]), split(spec[residue]))
        z.append(both[:block] + unturn(both[block:]))
    return butterfly(z, unturn)


def choose(flag, values, partner):
    return [jnp.where(flag == 0, values[q], values[partner[q]]) for q in range(RADIX)]


def x_kernel(plan, mode, partner, out_partner, out_rows, flag, *refs):
    refs = list(refs)

    def take(number):
        head = refs[:number]
        del refs[:number]
        return head

    inputs = take(RADIX)
    fh, fl, ih, il = take(4)
    state_in = take({"state": 0, "v": 1, "a": 2, "b": 2, "c": 1}[mode])
    coef = take({"state": 0, "v": 4, "a": 3, "b": 2, "c": 1}[mode])
    state_out = take({"state": 1, "v": 2, "a": 1, "b": 1, "c": 0}[mode])
    keep = None if mode in ("state", "c") else take(1)[0]
    fields = refs
    place = flag[0]
    loaded = [jnp.concatenate([r[0], r[1]], axis=1) for r in inputs]
    x = choose(place, loaded, partner)
    spec = x_forward_values(plan, x, fh, fl)
    count = plan.count
    fresh = []
    for residue in range(RADIX):
        rows = slice(residue * count, (residue + 1) * count)

        def read(ref):
            return jnp.concatenate([ref[0, rows, :], ref[1, rows, :]], axis=1)

        def factor(ref):
            return jnp.concatenate([ref[rows, :], ref[rows, :]], axis=1)

        def write(ref, value):
            ref[0, rows, :] = value[:, :LANES]
            ref[1, rows, :] = value[:, LANES:]

        term = spec[residue]
        if mode == "state":
            write(state_out[0], term)
            fresh.append(term)
        elif mode == "v":
            v = read(state_in[0])
            full, half, q, one = [factor(r) for r in coef]
            pushed = q * term
            a = half * v + pushed
            write(state_out[0], half * a - pushed)
            write(state_out[1], full * v + one * term)
            fresh.append(a)
        elif mode == "a":
            half, q, two = [factor(r) for r in coef]
            fresh.append(half * read(state_in[0]) + q * term)
            write(state_out[0], read(state_in[1]) + two * term)
        elif mode == "b":
            q, two = [factor(r) for r in coef]
            fresh.append(read(state_in[0]) + (2.0 * q) * term)
            write(state_out[0], read(state_in[1]) + two * term)
        else:
            fresh.append(read(state_in[0]) + factor(coef[0]) * term)

    def put(targets, values):
        values = choose(place, values, out_partner)
        for q in range(RADIX):
            which, row = out_rows[q]
            target = targets[which]
            target[0, row : row + plan.block, :] = values[q][:, :LANES]
            target[1, row : row + plan.block, :] = values[q][:, LANES:]

    for residue in range(RADIX):
        if keep is not None:
            write_spectrum(plan, keep, residue, fresh[residue])
    put(fields, x_inverse_values(plan, fresh, ih, il))


def write_spectrum(plan, ref, residue, value):
    rows = slice(residue * plan.count, (residue + 1) * plan.count)
    ref[0, rows, :] = value[:, :LANES]
    ref[1, rows, :] = value[:, LANES:]


def x_slope_kernel(plan, out_partner, out_rows, flag, spectrum, ih, il, kx, *fields):
    place = flag[0]
    fresh = []
    for residue in range(RADIX):
        rows = slice(residue * plan.count, (residue + 1) * plan.count)
        wave = kx[rows, :]
        fresh.append(jnp.concatenate([spectrum[0, rows, :] * wave, spectrum[1, rows, :] * wave], axis=1))
    values = choose(place, x_inverse_values(plan, fresh, ih, il), out_partner)
    for q in range(RADIX):
        which, row = out_rows[q]
        fields[which][0, row : row + plan.block, :] = values[q][:, :LANES]
        fields[which][1, row : row + plan.block, :] = values[q][:, LANES:]


SCALAR = pl.BlockSpec(memory_space=pltpu.SMEM)


def fixed(shape):
    return pl.BlockSpec(memory_space=pltpu.VMEM)


def params():
    return pltpu.CompilerParams(
        dimension_semantics=("arbitrary",), vmem_limit_bytes=VMEM_LIMIT
    )


def row_tile(rows):
    tile = min(rows, 256)
    return tile if rows % tile == 0 else rows


def pair_shape(rows, width):
    return jax.ShapeDtypeStruct((2, rows, width), F32)


def pair_spec(tile, width):
    return pl.BlockSpec((2, tile, width), lambda i: (0, i, 0))


def y_first(plan, flag, grid, forward):
    rows = grid.shape[0]
    tile = row_tile(rows)
    return pl.pallas_call(
        functools.partial(y_first_kernel, plan),
        name="y_first",
        grid=(rows // tile,),
        in_specs=[
            SCALAR,
            pl.BlockSpec((tile, plan.points), lambda i: (i, 0)),
            fixed(forward[0].shape),
            fixed(forward[1].shape),
        ],
        out_specs=[pair_spec(tile, plan.width)] * 2,
        out_shape=[pair_shape(rows, plan.width)] * 2,
        compiler_params=params(),
    )(flag, grid, *forward)


def y_middle(plan, flag, ky, fields, grad, forward):
    rows = fields[0].shape[1]
    tile = row_tile(rows)
    return pl.pallas_call(
        functools.partial(y_middle_kernel, plan),
        name="y_middle",
        grid=(rows // tile,),
        in_specs=[SCALAR, fixed(ky.shape)]
        + [pair_spec(tile, plan.width)] * 4
        + [fixed(t.shape) for t in (*grad, *forward)],
        out_specs=[pair_spec(tile, plan.width)] * 2,
        out_shape=[pair_shape(rows, plan.width)] * 2,
        compiler_params=params(),
    )(flag, ky, *fields, *grad, *forward)


def y_last(plan, flag, pieces, plain):
    rows = pieces[0].shape[1]
    tile = row_tile(rows)
    return pl.pallas_call(
        functools.partial(y_last_kernel, plan, len(pieces)),
        name="y_last",
        grid=(rows // tile,),
        in_specs=[SCALAR]
        + [pair_spec(tile, plan.width)] * len(pieces)
        + [fixed(t.shape) for t in plain],
        out_specs=pl.BlockSpec((tile, plan.points), lambda i: (i, 0)),
        out_shape=jax.ShapeDtypeStruct((rows, plan.points), F32),
        compiler_params=params(),
    )(flag, *pieces, *plain)


def x_stage(plan, mode, flag, inputs, partner, tables, state, coef, out_rows, out_partner, sizes):
    def rows_at(place):
        return pl.BlockSpec((2, plan.block, LANES), lambda i: (0, place, i))

    spectrum = pl.BlockSpec((2, plan.rows, LANES), lambda i: (0, 0, i))
    factor = pl.BlockSpec((plan.rows, LANES), lambda i: (0, i))
    kept = {"state": 1, "v": 3, "a": 2, "b": 2, "c": 0}[mode]
    return pl.pallas_call(
        functools.partial(x_kernel, plan, mode, partner, out_partner, out_rows),
        name="x_" + mode,
        grid=(plan.width // LANES,),
        in_specs=[SCALAR]
        + [rows_at(place) for unused_array, place in inputs]
        + [fixed(t.shape) for t in tables]
        + [spectrum] * len(state)
        + [factor] * len(coef),
        out_specs=[spectrum] * kept
        + [pl.BlockSpec((2, size, LANES), lambda i: (0, 0, i)) for size in sizes],
        out_shape=[pair_shape(plan.rows, plan.width)] * kept
        + [pair_shape(size, plan.width) for size in sizes],
        compiler_params=params(),
    )(flag, *[array for array, unused_place in inputs], *tables, *state, *coef)


def x_slope(plan, flag, spectrum, inverse, kx, out_rows, out_partner, sizes):
    return pl.pallas_call(
        functools.partial(x_slope_kernel, plan, out_partner, out_rows),
        name="x_slope",
        grid=(plan.width // LANES,),
        in_specs=[SCALAR, pl.BlockSpec((2, plan.rows, LANES), lambda i: (0, 0, i))]
        + [fixed(t.shape) for t in (*inverse, kx)],
        out_specs=[pl.BlockSpec((2, size, LANES), lambda i: (0, 0, i)) for size in sizes],
        out_shape=[pair_shape(size, plan.width) for size in sizes],
        compiler_params=params(),
    )(flag, spectrum, *inverse, kx)


def on_device(members, devices, field):
    plan = Plan(field.shape[1])
    rows = field.shape[0]
    half = devices // 2
    core = lax.axis_index("ens") % 2
    place = lax.axis_index("fft")
    core_flag = core.astype(jnp.int32).reshape(1)
    place_flag = place.astype(jnp.int32).reshape(1)
    side_flag = (place >= half).astype(jnp.int32).reshape(1)

    forward = y_forward_table(plan)
    grad, plain = y_inverse_tables(plan)
    x_forward, x_inverse = x_tables(plan)
    scale = WAVENUMBER_SCALE / plan.points
    wave_y = jnp.asarray(plan.ky.astype(np.float32) * np.float32(scale))
    wave_x = jnp.asarray(plan.kx.reshape(-1).astype(np.float32) * np.float32(scale))
    own_y = jnp.where(core == 0, wave_y[0], wave_y[1])
    kx = jnp.broadcast_to(wave_x[:, None], (plan.rows, LANES))
    ksq = (wave_x * wave_x)[:, None] + (own_y * own_y)[None, :]
    decay, decay_half, q_coef, f_one, f_two, f_three = coefficients(ksq)
    q_coef = -0.5 * q_coef
    f_one = -0.5 * f_one
    f_two = -f_two
    f_three = -0.5 * f_three

    def index(member, at):
        return member * devices + at

    def gather_pairs(k):
        pairs = []
        for base in range(0, members, 2):
            for which in range(2):
                for to_core in range(2):
                    source = (k + to_core * half) % devices
                    pairs.append((index(base + which, source), index(base + to_core, half - 1 + which)))
        return pairs

    sibling = [
        (index(m, at), index(m ^ 1, at)) for m in range(members) for at in range(devices)
    ]
    axes = ("ens", "fft")
    first, second = y_first(plan, side_flag, field, forward)
    pieces = [
        lax.ppermute(first if k < half else second, axes, gather_pairs(k)) for k in range(devices)
    ]
    coefs = (decay, decay_half, q_coef, f_one, f_two, f_three)
    pieces, coefs, kx, wave_y, grad, plain, x_forward, x_inverse = lax.optimization_barrier(
        (pieces, coefs, kx, wave_y, grad, plain, x_forward, x_inverse)
    )
    decay, decay_half, q_coef, f_one, f_two, f_three = coefs
    tables = (*x_forward, *x_inverse)
    per = rows // plan.block
    opposite = tuple((q + RADIX // 2) % RADIX for q in range(RADIX))
    beside = tuple(q ^ 1 for q in range(RADIX))
    part = plan.points // 4
    near = tuple((q % 2 * 2 + q // 4, q // 2 % 2 * plan.block) for q in range(RADIX))
    quarters = (part,) * 4

    def swap(value):
        return lax.ppermute(value, axes, sibling)

    def nonlinear(fields, spectrum, mode, state, coef):
        pa, pb, *p_out = fields
        p_in = [swap(value) for value in p_out]
        qa, qb, *q_out = x_slope(plan, core_flag, spectrum, x_inverse, kx, near, beside, quarters)
        q_in = [swap(value) for value in q_out]
        halves = []
        for h, (p, q) in enumerate(((pa, qa), (pb, qb))):
            own, send = y_middle(plan, core_flag, wave_y, (p, p_in[h], q, q_in[h]), grad, forward)
            halves.append((own, swap(send)))
        inputs = [(halves[q // 4][q % 2], q // 2 % 2) for q in range(RADIX)]
        if mode == "c":
            out_rows = tuple((q // per, q % per * plan.block) for q in range(RADIX))
            return x_stage(
                plan, mode, core_flag, inputs, beside, tables, state, coef, out_rows, opposite, (rows,) * devices
            )
        return x_stage(
            plan, mode, core_flag, inputs, beside, tables, state, coef, near, beside, quarters
        )

    inputs = [(pieces[q // per], q % per) for q in range(RADIX)]
    v, *fields = x_stage(
        plan, "state", core_flag, inputs, opposite, tables, (), (), near, beside, quarters
    )
    c_part, total, a, *fields = nonlinear(fields, v, "v", (v,), (decay, decay_half, q_coef, f_one))
    total, b, *fields = nonlinear(fields, a, "a", (v, total), (decay_half, q_coef, f_two))
    total, c, *fields = nonlinear(fields, b, "b", (c_part, total), (q_coef, f_two))
    outputs = nonlinear(fields, c, "c", (total,), (f_three,))
    received = [
        lax.ppermute(outputs[k], axes, [(to, source) for source, to in gather_pairs(k)])
        for k in range(devices)
    ]
    return y_last(plan, place_flag, received, plain)


def solution(mesh):
    members = mesh.shape["ens"]
    devices = mesh.shape["fft"]
    return jax.shard_map(
        functools.partial(on_device, members, devices),
        mesh=mesh,
        in_specs=(P(("ens", "fft"), None),),
        out_specs=P(("ens", "fft"), None),
        check_vma=False,
    )
```

```python
import functools
import math

import jax
import jax.numpy as jnp
import numpy as np
from jax import lax
from jax.experimental import pallas as pl
from jax.experimental.pallas import tpu as pltpu
from jax.sharding import PartitionSpec as P

STEP = 0.05
WAVENUMBER_SCALE = 8.0
RADIX = 8
Y_RADIX = 16
LANES = 128
ROOT = math.sqrt(0.5)
BIG = math.cos(math.pi / 8)
TINY = math.sin(math.pi / 8)
X_LIMIT = 36
Y_LIMIT = 22
SLOPE_LIMIT = 22
F32 = jnp.float32
BF16 = jnp.bfloat16


def phis(z):
    small = jnp.abs(z) < 1.0
    zs = jnp.where(small, z, 0.0)
    coeffs = [1.0 / math.factorial(n + 3) for n in range(16)]
    third = jnp.zeros_like(z) + coeffs[-1]
    for value in reversed(coeffs[:-1]):
        third = third * zs + value
    second = 0.5 + zs * third
    first = 1.0 + zs * second
    zl = jnp.where(small, -1.0, z)
    first_l = jnp.expm1(zl) / zl
    second_l = (first_l - 1.0) / zl
    third_l = (second_l - 0.5) / zl
    return (
        jnp.where(small, first, first_l),
        jnp.where(small, second, second_l),
        jnp.where(small, third, third_l),
    )


def coefficients(ksq):
    z = STEP * (ksq - ksq * ksq)
    half_one, unused_two, unused_three = phis(0.5 * z)
    one, two, three = phis(z)
    return (
        jnp.exp(z),
        jnp.exp(0.5 * z),
        0.5 * STEP * half_one,
        STEP * (one - 3.0 * two + 4.0 * three),
        STEP * (two - 2.0 * three),
        STEP * (4.0 * three - two),
    )


def round_up(value, step):
    return (value + step - 1) // step * step


class Plan:
    def __init__(self, points):
        self.points = points
        limit = points // 3
        signed = np.arange(-limit + 1, limit)
        self.y_block = points // Y_RADIX
        of_class = {r: signed[signed % Y_RADIX == r] for r in range(1, Y_RADIX // 2)}
        for r in (0, Y_RADIX // 2):
            of_class[r] = signed[(signed % Y_RADIX == r) & (signed >= 0)]
        self.groups = (((2,), (4,), (6,), (0, 8)), ((1,), (3,), (5,), (7,)))
        joined = [[np.concatenate([of_class[r] for r in group]) for group in one] for one in self.groups]
        self.used = max(len(one) for parity in joined for one in parity)
        self.tile = round_up(self.used, LANES)
        self.third = -(-self.used // 3)
        self.tiles = 3
        self.width = self.tiles * self.tile
        self.lane_ky = np.zeros((2, 4, self.tile), np.int32)
        self.lane_class = np.full((2, 4, self.tile), -1, np.int32)
        self.ky = np.zeros((2, self.width), np.int32)
        self.places = (self.used, 0, self.third)
        for parity in range(2):
            for group in range(3):
                one = joined[parity][group]
                self.lane_ky[parity, group, : len(one)] = one
                self.lane_class[parity, group, : len(one)] = one % Y_RADIX
                self.ky[parity, group * self.tile : group * self.tile + len(one)] = one
            for piece in range(3):
                one = joined[parity][3][piece * self.third : (piece + 1) * self.third]
                at = self.places[piece]
                self.lane_ky[parity, 3, at : at + len(one)] = one
                self.lane_class[parity, 3, at : at + len(one)] = one % Y_RADIX
                at = piece * self.tile + self.used
                self.ky[parity, at : at + len(one)] = one
        self.block = points // RADIX
        per_class = [signed[signed % RADIX == residue] for residue in range(RADIX)]
        self.count = round_up(max(len(one) for one in per_class), 16)
        self.kx = np.zeros((RADIX, self.count), np.int32)
        self.kx_live = np.zeros((RADIX, self.count), np.float32)
        for residue, one in enumerate(per_class):
            self.kx[residue, : len(one)] = one
            self.kx_live[residue, : len(one)] = 1.0
        self.rows = RADIX * self.count


def hi_lo(table):
    high = lax.reduce_precision(table, 8, 7)
    return high.astype(BF16), (table - high).astype(BF16)


def waves(points, left, right):
    product = (left * right) & (points - 1)
    angle = product.astype(F32) * (2.0 * math.pi / points)
    return jnp.cos(angle), jnp.sin(angle)


def y_parts(plan, xp, cos, sin):
    out = []
    for parity in range(2):
        for group in range(4):
            at = (parity * 4 + group) * plan.tile
            c, s = cos[:, at : at + plan.tile], sin[:, at : at + plan.tile]
            cls = plan.lane_class[parity, group]
            if group == 3 and parity == 0:
                low = (cls == 0).astype(np.float32)
                high = (cls == Y_RADIX // 2).astype(np.float32)
                out.append((True, c * low, s * low, c * high, s * high))
            else:
                live = (cls >= 0).astype(np.float32)
                out.append((False, c * live, s * live, None, None))
    return out


def y_forward_table(plan):
    n = np.arange(plan.y_block, dtype=np.int64)
    ky = plan.lane_ky.reshape(-1).astype(np.int64)
    angle = (n[:, None] * ky[None, :] % plan.points) * (2.0 * math.pi / plan.points)
    blocks = []
    for real, c, s, c8, s8 in y_parts(plan, np, np.cos(angle), np.sin(angle)):
        top = np.concatenate([c, -s], axis=1)
        low = np.concatenate([c8, -s8] if real else [s, c], axis=1)
        blocks.append(np.concatenate([top, low], axis=0))
    table = np.stack(blocks)
    high = table.astype(BF16)
    low = (table - high.astype(np.float64)).astype(BF16)
    return jnp.asarray(high), jnp.asarray(low)


def y_inverse_tables(plan):
    n = jnp.arange(plan.y_block, dtype=jnp.int32)
    ky = jnp.asarray(plan.lane_ky.reshape(-1))
    cos, sin = waves(plan.points, ky[:, None], n[None, :])
    weight = np.where(plan.lane_ky.reshape(-1) == 0, 1.0, 2.0) / (plan.points * plan.points)
    low = np.where(plan.lane_class == Y_RADIX // 2, 0.0, 1.0)
    low = np.where(plan.lane_class < 0, 0.0, low).reshape(-1) * weight
    high = np.where(plan.lane_class == Y_RADIX // 2, weight.reshape(plan.lane_class.shape), 0.0)
    real = np.zeros(plan.lane_class.shape, bool)
    real[0, 3] = True
    real = real.reshape(-1)
    low = jnp.asarray(low.astype(np.float32))[:, None]
    high = jnp.asarray(high.reshape(-1).astype(np.float32))[:, None]
    real = jnp.asarray(real)[:, None]
    c, s, ch, sh = cos * low, sin * low, cos * high, sin * high
    shape = (8, plan.tile, plan.y_block)

    def corner(complex_value, real_value):
        return jnp.where(real, real_value, complex_value).reshape(shape)

    def build(a, b, d, e):
        up = jnp.concatenate([a, b], axis=2)
        down = jnp.concatenate([d, e], axis=2)
        return hi_lo(jnp.concatenate([up, down], axis=1))

    plain = build(c.reshape(shape), corner(s, ch), (-s).reshape(shape), corner(c, -sh))
    grad = build((-s).reshape(shape), corner(c, -sh), (-c).reshape(shape), corner(-s, -ch))
    return grad, plain


def x_tables(plan):
    n = jnp.arange(plan.block, dtype=jnp.int32)
    kx = jnp.asarray(plan.kx)
    cos, sin = waves(plan.points, kx[:, :, None], n[None, None, :])
    live = jnp.asarray(plan.kx_live)[:, :, None]
    cos = cos * live
    sin = sin * live
    forward = jnp.concatenate([cos, sin], axis=1)
    inverse = jnp.concatenate([cos.transpose(0, 2, 1), sin.transpose(0, 2, 1)], axis=1)
    return hi_lo(forward), hi_lo(inverse)


def split(value):
    high = value.astype(BF16)
    return high, (value - high.astype(F32)).astype(BF16)


def dot(left, right):
    return jnp.dot(left, right, preferred_element_type=F32)


def dot3(left, right):
    lh, ll = left
    rh, rl = right
    return dot(lh, rh) + dot(lh, rl) + dot(ll, rh)


def real_forward(x):
    p = [x[q] + x[q + 4] for q in range(4)]
    m = [x[q] - x[q + 4] for q in range(4)]
    even = p[0] + p[2]
    odd = p[1] + p[3]
    minus = ROOT * (m[1] - m[3])
    plus = ROOT * (m[1] + m[3])
    return (
        even + odd,
        even - odd,
        (m[0] + minus, -m[2] - plus),
        (p[0] - p[2], p[3] - p[1]),
        (m[0] - minus, m[2] - plus),
    )


def real_inverse(z0, z4, z1, z2, z3):
    u, v = z0 + z4, z0 - z4
    even = [u + z2[0], v - z2[1], u - z2[0], v + z2[1]]
    s, t = z1[0] - z3[0], z1[1] + z3[1]
    odd = [z1[0] + z3[0], ROOT * (s - t), z3[1] - z1[1], -ROOT * (s + t)]
    return [even[q] + odd[q] for q in range(4)] + [even[q] - odd[q] for q in range(4)]


def lanes_of(value):
    return lax.broadcasted_iota(jnp.int32, value.shape, 1)


def y_forward_values(plan, x, table_hi, table_lo):
    p = [x[q] + x[q + 8] for q in range(8)]
    m = [x[q] - x[q + 8] for q in range(8)]
    z0, z8, z2, z4, z6 = real_forward(p)
    a = [m[q] - m[8 - q] for q in (1, 2, 3)]
    b = [m[q] + m[8 - q] for q in (1, 2, 3)]
    first, last = m[0] + ROOT * a[1], m[0] - ROOT * a[1]
    u, v = BIG * a[0] + TINY * a[2], TINY * a[0] - BIG * a[2]
    g, h = m[4] + ROOT * b[1], m[4] - ROOT * b[1]
    s, t = TINY * b[0] + BIG * b[2], BIG * b[0] - TINY * b[2]
    groups = [
        [z2, z4, z6, (z0, z8)],
        [(first + u, -g - s), (last + v, h - t), (last - v, -h - t), (first - u, g - s)],
    ]
    out = {}
    for parity in range(2):
        values = []
        for group in range(4):
            k = parity * 4 + group
            data = split(jnp.concatenate(groups[parity][group], axis=1))
            both = dot3(data, (table_hi[k], table_lo[k]))
            values.append((both[:, : plan.tile], both[:, plan.tile :]))
        lane = lanes_of(values[3][0])
        inside = (lane >= plan.used) & (lane < plan.used + plan.third)
        for tile in range(3):
            shift = (plan.used - plan.places[tile]) % plan.tile
            pair = []
            for part in range(2):
                extra = values[3][part]
                if shift:
                    extra = pltpu.roll(extra, shift, 1)
                pair.append(jnp.where(inside, extra, values[tile][part]))
            out[(parity, tile)] = tuple(pair)
    return out


def y_inverse_values(plan, tiles, table_hi, table_lo):
    z = []
    for parity in range(2):
        extra = []
        for part in range(2):
            value = [tiles[(parity, tile)][part] for tile in range(3)]
            lane = lanes_of(value[0])
            one = pltpu.roll(value[1], plan.tile - plan.used, 1)
            two = pltpu.roll(value[2], plan.tile - plan.used + plan.third, 1)
            extra.append(jnp.where(lane >= plan.used, value[0], jnp.where(lane < plan.third, one, two)))
        for group in range(4):
            k = parity * 4 + group
            pair = tuple(extra) if group == 3 else tiles[(parity, group)]
            both = dot3(split(jnp.concatenate(pair, axis=1)), (table_hi[k], table_lo[k]))
            z.append((both[:, : plan.y_block], both[:, plan.y_block :]))
    z2, z4, z6, (z0, z8), z1, z3, z5, z7 = z
    even = real_inverse(z0, z8, z2, z4, z6)
    r17, r35 = z1[0] + z7[0], z3[0] + z5[0]
    d17, d35 = z1[0] - z7[0], z3[0] - z5[0]
    i17, i35 = z1[1] + z7[1], z3[1] + z5[1]
    j17, j35 = z1[1] - z7[1], z3[1] - z5[1]
    c1, c2, c3 = BIG * d17 + TINY * d35, ROOT * (r17 - r35), TINY * d17 - BIG * d35
    s1, s2, s3 = TINY * i17 + BIG * i35, ROOT * (j17 + j35), BIG * i17 - TINY * i35
    odd = [r17 + r35, c1 - s1, c2 - s2, c3 - s3, j35 - j17, -c3 - s3, -c2 - s2, -c1 - s1]
    return [even[q] + odd[q] for q in range(8)] + [even[q] - odd[q] for q in range(8)]


def store_pair(plan, flag, out, first, second):
    for tile in range(plan.tiles):
        lanes = slice(tile * plan.tile, (tile + 1) * plan.tile)
        for part in range(2):
            even, odd = out[(0, tile)][part], out[(1, tile)][part]
            first[part, :, lanes] = jnp.where(flag == 0, even, odd)
            second[part, :, lanes] = jnp.where(flag == 0, odd, even)


def load_pair(plan, flag, own, other):
    out = {}
    for tile in range(plan.tiles):
        lanes = slice(tile * plan.tile, (tile + 1) * plan.tile)
        mine = (own[0, :, lanes], own[1, :, lanes])
        its = (other[0, :, lanes], other[1, :, lanes])
        out[(0, tile)] = tuple(jnp.where(flag == 0, a, b) for a, b in zip(mine, its))
        out[(1, tile)] = tuple(jnp.where(flag == 0, b, a) for a, b in zip(mine, its))
    return out


def y_first_kernel(plan, flag, grid, fh, fl, first, second):
    block = plan.y_block
    blocks = [grid[:, q * block : (q + 1) * block] for q in range(Y_RADIX)]
    store_pair(plan, flag[0], y_forward_values(plan, blocks, fh, fl), first, second)


def y_middle_kernel(plan, flag, ky, po, pr, qo, qr, gh, gl, fh, fl, first, second):
    gx = y_inverse_values(plan, load_pair(plan, flag[0], qo, qr), gh, gl)
    square = [value * value for value in gx]
    tiles = load_pair(plan, flag[0], po, pr)
    scaled = {}
    for (parity, tile), pair in tiles.items():
        row = ky[parity : parity + 1, tile * plan.tile : (tile + 1) * plan.tile]
        scaled[(parity, tile)] = tuple(value * row for value in pair)
    gy = y_inverse_values(plan, scaled, gh, gl)
    square = [one + two * two for one, two in zip(square, gy)]
    store_pair(plan, flag[0], y_forward_values(plan, square, fh, fl), first, second)


def y_last_kernel(plan, count, flag, *refs):
    received, (ph, plo, grid) = refs[:count], refs[count:]
    place = flag[0]
    tiles = {}
    for tile in range(plan.tiles):
        lanes = slice(tile * plan.tile, (tile + 1) * plan.tile)
        pairs = ([], [])
        for part in range(2):
            loaded = [r[part, :, lanes] for r in received]
            even, odd = loaded[0], loaded[count // 2]
            for k in range(1, count):
                even = jnp.where(place == k, loaded[k], even)
                odd = jnp.where(place == k, loaded[(k + count // 2) % count], odd)
            pairs[0].append(even)
            pairs[1].append(odd)
        tiles[(0, tile)] = tuple(pairs[0])
        tiles[(1, tile)] = tuple(pairs[1])
    blocks = y_inverse_values(plan, tiles, ph, plo)
    for q in range(Y_RADIX):
        grid[:, q * plan.y_block : (q + 1) * plan.y_block] = blocks[q]


def turn(value):
    return jnp.concatenate([value[:, LANES:], -value[:, :LANES]], axis=1)


def unturn(value):
    return jnp.concatenate([-value[:, LANES:], value[:, :LANES]], axis=1)


def butterfly(x, rotate):
    p = [x[q] + x[q + 4] for q in range(4)]
    m = [x[q] - x[q + 4] for q in range(4)]
    s0, s1 = p[0] + p[2], p[1] + p[3]
    d0, d1 = p[0] - p[2], rotate(p[1] - p[3])
    a = ROOT * (m[1] - m[3])
    b = rotate(ROOT * (m[1] + m[3]))
    c = rotate(m[2])
    top, low = m[0] + c, m[0] - c
    plus, minus = a + b, a - b
    return [
        s0 + s1,
        top + plus,
        d0 + d1,
        low - minus,
        s0 - s1,
        top - plus,
        d0 - d1,
        low + minus,
    ]


def x_forward_values(plan, x, table_hi, table_lo):
    count = plan.count
    out = []
    for residue, value in enumerate(butterfly(x, turn)):
        both = dot3((table_hi[residue], table_lo[residue]), split(value))
        out.append(both[:count] + turn(both[count:]))
    return out


def x_inverse_values(plan, spec, table_hi, table_lo):
    block = plan.block
    z = []
    for residue in range(RADIX):
        both = dot3((table_hi[residue], table_lo[residue]), split(spec[residue]))
        z.append(both[:block] + unturn(both[block:]))
    return butterfly(z, unturn)


def choose(flag, values, partner):
    return [jnp.where(flag == 0, values[q], values[partner[q]]) for q in range(RADIX)]


def x_kernel(plan, mode, partner, out_partner, out_rows, flag, *refs):
    refs = list(refs)

    def take(number):
        head = refs[:number]
        del refs[:number]
        return head

    inputs = take(RADIX)
    fh, fl, ih, il = take(4)
    state_in = take({"state": 0, "v": 1, "a": 2, "b": 2, "c": 1}[mode])
    coef = take({"state": 0, "v": 4, "a": 3, "b": 2, "c": 1}[mode])
    state_out = take({"state": 1, "v": 2, "a": 1, "b": 1, "c": 0}[mode])
    keep = None if mode in ("state", "c") else take(1)[0]
    fields = refs
    place = flag[0]
    loaded = [jnp.concatenate([r[0], r[1]], axis=1) for r in inputs]
    x = choose(place, loaded, partner)
    spec = x_forward_values(plan, x, fh, fl)
    count = plan.count
    fresh = []
    for residue in range(RADIX):
        rows = slice(residue * count, (residue + 1) * count)

        def read(ref):
            return jnp.concatenate([ref[0, rows, :], ref[1, rows, :]], axis=1)

        def factor(ref):
            return jnp.concatenate([ref[rows, :], ref[rows, :]], axis=1)

        def write(ref, value):
            ref[0, rows, :] = value[:, :LANES]
            ref[1, rows, :] = value[:, LANES:]

        term = spec[residue]
        if mode == "state":
            write(state_out[0], term)
            fresh.append(term)
        elif mode == "v":
            v = read(state_in[0])
            full, half, q, one = [factor(r) for r in coef]
            pushed = q * term
            a = half * v + pushed
            write(state_out[0], half * a - pushed)
            write(state_out[1], full * v + one * term)
            fresh.append(a)
        elif mode == "a":
            half, q, two = [factor(r) for r in coef]
            fresh.append(half * read(state_in[0]) + q * term)
            write(state_out[0], read(state_in[1]) + two * term)
        elif mode == "b":
            q, two = [factor(r) for r in coef]
            fresh.append(read(state_in[0]) + (2.0 * q) * term)
            write(state_out[0], read(state_in[1]) + two * term)
        else:
            fresh.append(read(state_in[0]) + factor(coef[0]) * term)

    def put(targets, values):
        values = choose(place, values, out_partner)
        for q in range(RADIX):
            which, row = out_rows[q]
            target = targets[which]
            target[0, row : row + plan.block, :] = values[q][:, :LANES]
            target[1, row : row + plan.block, :] = values[q][:, LANES:]

    for residue in range(RADIX):
        if keep is not None:
            write_spectrum(plan, keep, residue, fresh[residue])
    put(fields, x_inverse_values(plan, fresh, ih, il))


def write_spectrum(plan, ref, residue, value):
    rows = slice(residue * plan.count, (residue + 1) * plan.count)
    ref[0, rows, :] = value[:, :LANES]
    ref[1, rows, :] = value[:, LANES:]


def x_slope_kernel(plan, out_partner, out_rows, flag, spectrum, ih, il, kx, *fields):
    place = flag[0]
    fresh = []
    for residue in range(RADIX):
        rows = slice(residue * plan.count, (residue + 1) * plan.count)
        wave = kx[rows, :]
        fresh.append(jnp.concatenate([spectrum[0, rows, :] * wave, spectrum[1, rows, :] * wave], axis=1))
    values = choose(place, x_inverse_values(plan, fresh, ih, il), out_partner)
    for q in range(RADIX):
        which, row = out_rows[q]
        fields[which][0, row : row + plan.block, :] = values[q][:, :LANES]
        fields[which][1, row : row + plan.block, :] = values[q][:, LANES:]


SCALAR = pl.BlockSpec(memory_space=pltpu.SMEM)


def fixed(shape):
    return pl.BlockSpec(memory_space=pltpu.VMEM)


def params(limit):
    return pltpu.CompilerParams(
        dimension_semantics=("arbitrary",), vmem_limit_bytes=limit * 1024 * 1024
    )


def row_tile(rows):
    tile = min(rows, 256)
    return tile if rows % tile == 0 else rows


def pair_shape(rows, width):
    return jax.ShapeDtypeStruct((2, rows, width), F32)


def pair_spec(tile, width):
    return pl.BlockSpec((2, tile, width), lambda i: (0, i, 0))


def y_first(plan, flag, grid, forward):
    rows = grid.shape[0]
    tile = row_tile(rows)
    return pl.pallas_call(
        functools.partial(y_first_kernel, plan),
        name="y_first",
        grid=(rows // tile,),
        in_specs=[
            SCALAR,
            pl.BlockSpec((tile, plan.points), lambda i: (i, 0)),
            fixed(forward[0].shape),
            fixed(forward[1].shape),
        ],
        out_specs=[pair_spec(tile, plan.width)] * 2,
        out_shape=[pair_shape(rows, plan.width)] * 2,
        compiler_params=params(Y_LIMIT),
    )(flag, grid, *forward)


def y_middle(plan, flag, ky, fields, grad, forward):
    rows = fields[0].shape[1]
    tile = row_tile(rows)
    return pl.pallas_call(
        functools.partial(y_middle_kernel, plan),
        name="y_middle",
        grid=(rows // tile,),
        in_specs=[SCALAR, fixed(ky.shape)]
        + [pair_spec(tile, plan.width)] * 4
        + [fixed(t.shape) for t in (*grad, *forward)],
        out_specs=[pair_spec(tile, plan.width)] * 2,
        out_shape=[pair_shape(rows, plan.width)] * 2,
        compiler_params=params(Y_LIMIT),
    )(flag, ky, *fields, *grad, *forward)


def y_last(plan, flag, pieces, plain):
    rows = pieces[0].shape[1]
    tile = row_tile(rows)
    return pl.pallas_call(
        functools.partial(y_last_kernel, plan, len(pieces)),
        name="y_last",
        grid=(rows // tile,),
        in_specs=[SCALAR]
        + [pair_spec(tile, plan.width)] * len(pieces)
        + [fixed(t.shape) for t in plain],
        out_specs=pl.BlockSpec((tile, plan.points), lambda i: (i, 0)),
        out_shape=jax.ShapeDtypeStruct((rows, plan.points), F32),
        compiler_params=params(Y_LIMIT),
    )(flag, *pieces, *plain)


def x_stage(plan, mode, flag, inputs, partner, tables, state, coef, out_rows, out_partner, sizes):
    def rows_at(place):
        return pl.BlockSpec((2, plan.block, LANES), lambda i: (0, place, i))

    spectrum = pl.BlockSpec((2, plan.rows, LANES), lambda i: (0, 0, i))
    factor = pl.BlockSpec((plan.rows, LANES), lambda i: (0, i))
    kept = {"state": 1, "v": 3, "a": 2, "b": 2, "c": 0}[mode]
    return pl.pallas_call(
        functools.partial(x_kernel, plan, mode, partner, out_partner, out_rows),
        name="x_" + mode,
        grid=(plan.width // LANES,),
        in_specs=[SCALAR]
        + [rows_at(place) for unused_array, place in inputs]
        + [fixed(t.shape) for t in tables]
        + [spectrum] * len(state)
        + [factor] * len(coef),
        out_specs=[spectrum] * kept
        + [pl.BlockSpec((2, size, LANES), lambda i: (0, 0, i)) for size in sizes],
        out_shape=[pair_shape(plan.rows, plan.width)] * kept
        + [pair_shape(size, plan.width) for size in sizes],
        compiler_params=params(X_LIMIT),
    )(flag, *[array for array, unused_place in inputs], *tables, *state, *coef)


def x_slope(plan, flag, spectrum, inverse, kx, out_rows, out_partner, sizes):
    return pl.pallas_call(
        functools.partial(x_slope_kernel, plan, out_partner, out_rows),
        name="x_slope",
        grid=(plan.width // LANES,),
        in_specs=[SCALAR, pl.BlockSpec((2, plan.rows, LANES), lambda i: (0, 0, i))]
        + [fixed(t.shape) for t in (*inverse, kx)],
        out_specs=[pl.BlockSpec((2, size, LANES), lambda i: (0, 0, i)) for size in sizes],
        out_shape=[pair_shape(size, plan.width) for size in sizes],
        compiler_params=params(SLOPE_LIMIT),
    )(flag, spectrum, *inverse, kx)


def on_device(members, devices, field):
    plan = Plan(field.shape[1])
    rows = field.shape[0]
    half = devices // 2
    core = lax.axis_index("ens") % 2
    place = lax.axis_index("fft")
    core_flag = core.astype(jnp.int32).reshape(1)
    place_flag = place.astype(jnp.int32).reshape(1)
    side_flag = (place >= half).astype(jnp.int32).reshape(1)

    forward = y_forward_table(plan)
    grad, plain = y_inverse_tables(plan)
    x_forward, x_inverse = x_tables(plan)
    scale = WAVENUMBER_SCALE / plan.points
    wave_y = jnp.asarray(plan.ky.astype(np.float32) * np.float32(scale))
    wave_x = jnp.asarray(plan.kx.reshape(-1).astype(np.float32) * np.float32(scale))
    own_y = jnp.where(core == 0, wave_y[0], wave_y[1])
    kx = jnp.broadcast_to(wave_x[:, None], (plan.rows, LANES))
    ksq = (wave_x * wave_x)[:, None] + (own_y * own_y)[None, :]
    decay, decay_half, q_coef, f_one, f_two, f_three = coefficients(ksq)
    q_coef = -0.5 * q_coef
    f_one = -0.5 * f_one
    f_two = -f_two
    f_three = -0.5 * f_three

    def index(member, at):
        return member * devices + at

    def gather_pairs(k):
        pairs = []
        for base in range(0, members, 2):
            for which in range(2):
                for to_core in range(2):
                    source = (k + to_core * half) % devices
                    pairs.append((index(base + which, source), index(base + to_core, half - 1 + which)))
        return pairs

    sibling = [
        (index(m, at), index(m ^ 1, at)) for m in range(members) for at in range(devices)
    ]
    axes = ("ens", "fft")
    first, second = y_first(plan, side_flag, field, forward)
    pieces = [
        lax.ppermute(first if k < half else second, axes, gather_pairs(k)) for k in range(devices)
    ]
    coefs = (decay, decay_half, q_coef, f_one, f_two, f_three)
    pieces, coefs, kx, wave_y, grad, plain, x_forward, x_inverse = lax.optimization_barrier(
        (pieces, coefs, kx, wave_y, grad, plain, x_forward, x_inverse)
    )
    decay, decay_half, q_coef, f_one, f_two, f_three = coefs
    tables = (*x_forward, *x_inverse)
    per = rows // plan.block
    opposite = tuple((q + RADIX // 2) % RADIX for q in range(RADIX))
    beside = tuple(q ^ 1 for q in range(RADIX))
    part = plan.points // 4
    near = tuple((q % 2 * 2 + q // 4, q // 2 % 2 * plan.block) for q in range(RADIX))
    quarters = (part,) * 4

    def swap(value):
        return lax.ppermute(value, axes, sibling)

    def nonlinear(fields, spectrum, mode, state, coef):
        pa, pb, *p_out = fields
        p_in = [swap(value) for value in p_out]
        qa, qb, *q_out = x_slope(plan, core_flag, spectrum, x_inverse, kx, near, beside, quarters)
        q_in = [swap(value) for value in q_out]
        halves = []
        for h, (p, q) in enumerate(((pa, qa), (pb, qb))):
            own, send = y_middle(plan, core_flag, wave_y, (p, p_in[h], q, q_in[h]), grad, forward)
            halves.append((own, swap(send)))
        inputs = [(halves[q // 4][q % 2], q // 2 % 2) for q in range(RADIX)]
        if mode == "c":
            out_rows = tuple((q // per, q % per * plan.block) for q in range(RADIX))
            return x_stage(
                plan, mode, core_flag, inputs, beside, tables, state, coef, out_rows, opposite, (rows,) * devices
            )
        return x_stage(
            plan, mode, core_flag, inputs, beside, tables, state, coef, near, beside, quarters
        )

    inputs = [(pieces[q // per], q % per) for q in range(RADIX)]
    v, *fields = x_stage(
        plan, "state", core_flag, inputs, opposite, tables, (), (), near, beside, quarters
    )
    c_part, total, a, *fields = nonlinear(fields, v, "v", (v,), (decay, decay_half, q_coef, f_one))
    total, b, *fields = nonlinear(fields, a, "a", (v, total), (decay_half, q_coef, f_two))
    total, c, *fields = nonlinear(fields, b, "b", (c_part, total), (q_coef, f_two))
    outputs = nonlinear(fields, c, "c", (total,), (f_three,))
    received = [
        lax.ppermute(outputs[k], axes, [(to, source) for source, to in gather_pairs(k)])
        for k in range(devices)
    ]
    return y_last(plan, place_flag, received, plain)


def solution(mesh):
    members = mesh.shape["ens"]
    devices = mesh.shape["fft"]
    return jax.shard_map(
        functools.partial(on_device, members, devices),
        mesh=mesh,
        in_specs=(P(("ens", "fft"), None),),
        out_specs=P(("ens", "fft"), None),
        check_vma=False,
    )
```
